32 devices in a mesh: pipe: 2 (over core), tensor: 2 (over x), expert: 8 (over z, y).
Axes of the slice: x: 2, y: 2, z: 4, core: 2. Of those that a mesh axis runs over, the one named last changes fastest.
Arguments:
- tokens: bfloat16 [3, 384, 4096], P(None, 'expert', 'tensor'), may hold values from -36 to 36
- norm_gain: float32 [2, 4096], P('pipe'), may hold values from 0.1 to 1.9
- shared_gate: bfloat16 [2, 4096, 1024], P('pipe', 'expert', 'tensor'), may hold values from -0.09375 to 0.09375
- shared_up: bfloat16 [2, 4096, 1024], P('pipe', 'expert', 'tensor'), may hold values from -0.09375 to 0.09375
- shared_down: bfloat16 [2, 1024, 4096], P('pipe', 'tensor', 'expert'), may hold values from -0.1875 to 0.1875
- expert_gate: bfloat16 [2, 8, 4096, 1024], P('pipe', 'expert', None, 'tensor'), may hold values from -0.09375 to 0.09375
- expert_up: bfloat16 [2, 8, 4096, 1024], P('pipe', 'expert', None, 'tensor'), may hold values from -0.09375 to 0.09375
- expert_down: bfloat16 [2, 8, 1024, 4096], P('pipe', 'expert', 'tensor'), may hold values from -0.1875 to 0.1875
- expert_ids: int32 [2, 3, 384, 8], P('pipe', None, 'expert'), may hold values from 0 to 255, as said below
- expert_slots: int32 [2, 3, 384, 8], P('pipe', None, 'expert'), may hold values from -1 to 2, as said below
- route_weights: float32 [2, 3, 384, 8], P('pipe', None, 'expert'), may hold values from 0.1 to 1
Outputs:
- states: bfloat16 [2, 3, 384, 4096], P('pipe', None, 'expert', 'tensor')
The draws below stay inside these ranges and needn't reach their ends.
Inputs may be any that keep to these rules, and one draw needn't show every extreme that they name: `expert_ids`: the 8 ids of a token are distinct. Ids of 8 and above name experts that are not held and add nothing. `expert_slots`: for a choice whose id is below 8: the number of earlier choices (earlier tokens, or lower k of the same token) of the same block of 48 tokens, same layer and microbatch, that name the same expert, if that number is below 3; otherwise -1. For ids of 8 and above: -1.
All inputs are finite; a program needn't handle non-finite values.
Results may differ from the reference program's by a relative error of at most 0.0085.
Values may be sent and summed in bfloat16 or wider, within the bound.
A program may use at most 64 MiB of HBM per device.

```python
import math
import jax
import jax.numpy as jnp
from jax import lax

D = 4096
FE = 1024
FS = 1024
ROUTED = 256
TOP = 8
CAP = 3
TE = 48
MB = 3
LAYERS = 2
HELD = 8
FE_DEV = 512
TOKENS = 384
N_TENSOR = 2


def route_table(key):
    subkeys = jax.random.split(jax.random.fold_in(key, 7001), 4)
    blocks = TOKENS // TE
    jitter = jax.random.randint(subkeys[0], (LAYERS, MB, TOKENS, ROUTED), 0, 2 ** 20, dtype=jnp.int32)
    popular = jax.random.randint(subkeys[1], (LAYERS, MB, 1, ROUTED), 0, 2, dtype=jnp.int32) * 2 ** 17
    hot_expert = jax.random.randint(subkeys[2], (LAYERS, MB, 1, 1), 0, HELD, dtype=jnp.int32)
    shuffle = jax.random.randint(subkeys[3], (LAYERS, MB, blocks, TE), 0, 2 ** 30, dtype=jnp.int32)
    position = jnp.argsort(jnp.argsort(shuffle, axis=-1, stable=True), axis=-1, stable=True)
    forced = (position < CAP + 1).reshape(LAYERS, MB, TOKENS, 1)
    column = jnp.arange(ROUTED, dtype=jnp.int32)
    lifted = jnp.where(forced & (column == hot_expert), 2 ** 21, 0).astype(jnp.int32)
    scores = (jitter + popular + lifted) * ROUTED + column
    chosen = lax.top_k(scores, TOP)[1].astype(jnp.int32)
    flat = chosen.reshape(LAYERS, MB, blocks, TE * TOP)
    in_window = flat < HELD
    matches = ((flat[..., None] == jnp.arange(HELD, dtype=jnp.int32)) & in_window[..., None]).astype(jnp.int32)
    earlier = jnp.cumsum(matches, axis=-2) - matches
    counted = jnp.sum(earlier * matches, axis=-1)
    slot_rank = jnp.where(in_window & (counted < CAP), counted, -1).astype(jnp.int32)
    return (chosen, slot_rank.reshape(LAYERS, MB, TOKENS, TOP))


def draw_expert_ids(key, part):
    return route_table(key)[0]


def draw_expert_slots(key, part):
    return route_table(key)[1]


def draw_tokens(key, part):
    subkeys = jax.random.split(jax.random.fold_in(key, 31), 3)
    row_scale = jnp.exp(jax.random.uniform(subkeys[0], (MB, TOKENS, 1), jnp.float32, jnp.log(0.3), jnp.log(3.0)))
    column_scale = jnp.exp(jax.random.uniform(subkeys[1], (1, 1, D), jnp.float32, jnp.log(0.3), jnp.log(3.0)))
    entries = jnp.clip(jax.random.normal(subkeys[2], (MB, TOKENS, D), jnp.float32), -4.0, 4.0)
    return jnp.clip(entries * row_scale * column_scale, -36.0, 36.0).astype(jnp.bfloat16)


def steps_of(rng, shape, cuts, smallest, top_value):
    loudness, own = 1.0, jax.random.fold_in(rng, 6)
    for axis_at, blocks in cuts:
        heights = jnp.exp(jax.random.uniform(jax.random.fold_in(own, axis_at), (blocks,), jnp.float32, smallest / len(cuts), top_value / len(cuts)))
        loudness = loudness * jnp.repeat(heights, shape[axis_at] // blocks).reshape([-1 if axis == axis_at else 1 for axis in range(len(shape))])
    return loudness


def bell_draw(own_key, extent, spread, most, cuts=(), held_as=jnp.bfloat16):
    loudness = steps_of(own_key, extent, cuts, -0.22, 0.18) if cuts else 1.0
    array = jax.random.normal(own_key, extent, jnp.float32) * spread * loudness
    return jnp.minimum(jnp.maximum(array, -most), most).astype(held_as)


def setup_inputs(seed: int = 0) -> dict:
    key_of = jax.random.split(jax.random.key(seed), 12)
    return {
        "tokens": draw_tokens(jax.random.fold_in(key_of[11], 71), 0),
        "norm_gain": jnp.clip(1.0 + 0.18 * jax.random.normal(key_of[1], (LAYERS, D), jnp.float32), 0.1, 1.9),
        "shared_gate": bell_draw(key_of[2], (LAYERS, D, FS), D ** -0.5, 0.09375, ((0, 2), (1, 8), (2, 2))),
        "shared_up": bell_draw(key_of[3], (LAYERS, D, FS), D ** -0.5, 0.09375, ((0, 2), (1, 8), (2, 2))),
        "shared_down": bell_draw(key_of[4], (LAYERS, FS, D), FS ** -0.5, 0.1875, ((0, 2), (1, 2), (2, 8))),
        "expert_gate": bell_draw(key_of[5], (LAYERS, HELD, D, FE), D ** -0.5, 0.09375, ((0, 2), (1, 8), (3, 2))),
        "expert_up": bell_draw(key_of[6], (LAYERS, HELD, D, FE), D ** -0.5, 0.09375, ((0, 2), (1, 8), (3, 2))),
        "expert_down": bell_draw(key_of[7], (LAYERS, HELD, FE, D), FE ** -0.5, 0.1875, ((0, 2), (1, 8), (2, 2))),
        "expert_ids": draw_expert_ids(jax.random.fold_in(key_of[11], 71), 0),
        "expert_slots": draw_expert_slots(jax.random.fold_in(key_of[11], 71), 0),
        "route_weights": jnp.clip(jnp.exp(math.log(1.0) - 2.3025851 * jax.random.uniform(key_of[10], (LAYERS, MB, TOKENS, TOP), jnp.float32) ** steps_of(key_of[10], (LAYERS, MB, TOKENS, TOP), ((0, 2), (2, 8)), -0.2, 0.2)), 0.1, 1.0),
    }


def product(left, right):
    return jnp.dot(left, right, preferred_element_type=jnp.float32)

def apply_layer(state, gain, sh_gate, sh_up, sh_down, ex_gate, ex_up, ex_down, route_ids, slot_rank, weights):
    values = state.astype(jnp.float32)
    inverse_rms = lax.rsqrt(lax.optimization_barrier(jnp.mean(values * values, axis=-1, keepdims=True)) + 1e-06)
    normed = (values * inverse_rms * gain).astype(jnp.bfloat16)
    shared_hidden = (jax.nn.silu(product(normed, sh_gate)) * product(normed, sh_up)).astype(jnp.bfloat16)
    shared_out = product(shared_hidden, sh_down)
    valid = (route_ids < HELD) & (slot_rank >= 0)
    slot_code = jnp.where(valid, route_ids * CAP + slot_rank, -1).astype(jnp.int32)
    blocks = TOKENS // TE
    code_blocks = slot_code.reshape(blocks, TE, TOP)
    slot_range = jnp.arange(HELD * CAP, dtype=jnp.int32)
    picker = jnp.any(code_blocks[:, None, :, :] == slot_range[None, :, None, None], axis=3).astype(jnp.float32)
    buffers = jnp.einsum('bjt,btd->bjd', picker, normed.reshape(blocks, TE, D).astype(jnp.float32)).astype(jnp.bfloat16)
    expert_rows = buffers.reshape(blocks, HELD, CAP, D).transpose(1, 0, 2, 3).reshape(HELD, blocks * CAP, D)

    def one_expert(operands):
        rows, w_gate, w_up, w_down = operands
        hidden = (jax.nn.silu(product(rows, w_gate)) * product(rows, w_up)).astype(jnp.bfloat16)
        summed = jnp.zeros((rows.shape[0], D), jnp.float32)
        for group in range(N_TENSOR):
            part = product(hidden[:, group * FE_DEV:(group + 1) * FE_DEV], w_down[group * FE_DEV:(group + 1) * FE_DEV]).astype(jnp.bfloat16)
            part = lax.optimization_barrier(part)
            summed = summed + part.astype(jnp.float32)
        return summed
    outputs = lax.map(one_expert, (expert_rows, ex_gate, ex_up, ex_down))
    returned = outputs.reshape(HELD, blocks, CAP, D).transpose(1, 0, 2, 3).reshape(blocks, HELD * CAP, D)
    index = jnp.maximum(code_blocks, 0).reshape(blocks, TE * TOP)[:, :, None]
    picked = jnp.take_along_axis(returned, index, axis=1).reshape(TOKENS, TOP, D)
    route_share = jnp.where(slot_code >= 0, weights, jnp.float32(0.0))
    routed = lax.optimization_barrier(jnp.sum(route_share[:, :, None] * picked, axis=1))
    return (values + shared_out + routed).astype(jnp.bfloat16)

def reference(tokens, norm_gain, shared_gate, shared_up, shared_down, expert_gate, expert_up, expert_down, expert_ids, expert_slots, route_weights):
    states = []
    for layer_index in range(LAYERS):
        layer_out = []
        for batch_index in range(MB):
            if layer_index == 0:
                state = tokens[batch_index]
            else:
                state = states[layer_index - 1][batch_index]
            layer_out.append(apply_layer(state, norm_gain[layer_index], shared_gate[layer_index], shared_up[layer_index], shared_down[layer_index], expert_gate[layer_index], expert_up[layer_index], expert_down[layer_index], expert_ids[layer_index, batch_index], expert_slots[layer_index, batch_index], route_weights[layer_index, batch_index]))
        states.append(jnp.stack(layer_out))
    return jnp.stack(states)
```

```python
import functools

import jax
import jax.numpy as jnp
from jax import lax
from jax.experimental import pallas as pl
from jax.experimental.pallas import tpu as pltpu
from jax.sharding import PartitionSpec as P

CAP = 3
MESH = pl.DeviceIdType.MESH
F32 = jnp.float32
BF16 = jnp.bfloat16


def product(left, right):
    return jnp.dot(left, right, preferred_element_type=F32)


def silu(value):
    return value / (1.0 + jnp.exp(-value))


def layer_kernel(
    ne, nt,
    x_hbm, gain, picker, combine, sg_hbm, su_hbm, sd_hbm, eg_hbm, eu_hbm, ed_hbm,
    out,
    xs, xn, sg, su, sd, eg, eu, ed,
    outg, arr, outc, ret, g_acc, u_acc, hid, eg_acc, eu_acc, ehid, y, rs, res,
    w_send, w_recv, d_send, d_recv, x_send, x_recv, a_send, a_recv, b_send, b_recv,
    r_send, r_recv, p_send, p_recv, own_sem, exp_sem, x_sem, go_sem,
):
    pipe = lax.axis_index("pipe")
    ten = lax.axis_index("tensor")
    me = lax.axis_index("expert")
    spt = ne // nt
    T, Ds = xs.shape[1], xs.shape[2]
    F = sg.shape[2]
    rows = outg.shape[1]
    half = F // 2
    base = ten * spt

    odd = me % 2
    pos = (1 - odd) * (me // 2) + odd * (ne - 1 - me // 2)

    def at(p):
        p = (p + 2 * ne) % ne
        upper = p // (ne // 2)
        return (1 - upper) * (2 * p) + upper * (2 * (ne - 1 - p) + 1)

    def remote(src, dst, send, recv, **device):
        return pltpu.make_async_remote_copy(
            src_ref=src, dst_ref=dst, send_sem=send, recv_sem=recv,
            device_id=device, device_id_type=MESH,
        )

    barrier = pltpu.get_barrier_semaphore()
    for k in range(1, ne):
        pl.semaphore_signal(barrier, inc=1, device_id={"expert": (me + k) % ne}, device_id_type=MESH)
    for k in range(1, nt):
        pl.semaphore_signal(barrier, inc=1, device_id={"tensor": (ten + k) % nt}, device_id_type=MESH)
    pl.semaphore_signal(barrier, inc=1, device_id={"pipe": 1 - pipe}, device_id_type=MESH)

    own = [
        pltpu.make_async_copy(sg_hbm, sg.at[me], own_sem.at[0]),
        pltpu.make_async_copy(su_hbm, su.at[me], own_sem.at[1]),
        pltpu.make_async_copy(sd_hbm, sd.at[me], own_sem.at[2]),
    ]
    for copy in own:
        copy.start()
    x_in = [
        pltpu.make_async_copy(x_hbm.at[:, pl.ds(i * Ds, Ds)], xs.at[base + i], x_sem.at[i])
        for i in range(spt)
    ]

    @pl.when(pipe == 0)
    def _():
        for copy in x_in:
            copy.start()

    experts = [
        pltpu.make_async_copy(eg_hbm, eg, exp_sem.at[0]),
        pltpu.make_async_copy(eu_hbm, eu, exp_sem.at[1]),
        pltpu.make_async_copy(ed_hbm, ed, exp_sem.at[2]),
    ]
    for copy in experts:
        copy.start()
    pl.semaphore_wait(barrier, ne - 1 + nt - 1 + 1)

    right, left = at(pos + 1), at(pos - 1)

    def gate_copy(s):
        block = sg.at[at(pos - s)]
        return remote(block, block, w_send.at[0, s], w_recv.at[0, s], expert=right)

    def up_copy(s):
        block = su.at[at(pos + s)]
        return remote(block, block, w_send.at[1, s], w_recv.at[1, s], expert=left)

    def down_a(s):
        block = sd.at[at(pos - s), pl.ds(0, half)]
        return remote(block, block, d_send.at[0, s], d_recv.at[0, s], expert=right)

    def down_b(s):
        block = sd.at[at(pos + s), pl.ds(half, half)]
        return remote(block, block, d_send.at[1, s], d_recv.at[1, s], expert=left)

    def ring(s):
        for group in ((gate_copy, up_copy), (down_a, down_b)):
            for make in group:
                make(s).wait_recv()
                if s + 1 < ne - 1:
                    make(s + 1).start()

    @pl.when(pipe == 1)
    def _():
        pl.semaphore_wait(go_sem, 1)

    for copy in own:
        copy.wait()
    for make in (gate_copy, up_copy, down_a, down_b):
        make(0).start()

    @pl.when(pipe == 0)
    def _():
        for copy in x_in:
            copy.wait()

    @pl.when(pipe == 1)
    def _():
        for i in range(spt):
            block = xs.at[base + i]
            remote(block, block, p_send.at[i], p_recv.at[i], pipe=1 - pipe).wait_recv()

    def x_copy(k, i):
        block = xs.at[base + i]
        return remote(block, block, x_send.at[k - 1, i], x_recv.at[k - 1, i], tensor=(ten + k) % nt)

    for k in range(1, nt):
        for i in range(spt):
            x_copy(k, i).start()
    ring(0)
    for k in range(1, nt):
        for i in range(spt):
            x_copy(k, i).wait_recv()

    def squares(j, total):
        v = xs[j].astype(F32)
        return total + jnp.sum(v * v, axis=-1, keepdims=True)

    total = lax.fori_loop(0, ne, squares, jnp.zeros((T, 1), F32))
    inverse = lax.rsqrt(total / (ne * Ds) + 1e-06)

    def normalise(j, carry):
        v = (xs[j].astype(F32) * inverse * gain[j]).astype(BF16)
        xn[j] = v
        sent = product(picker[...], v).astype(BF16).reshape(ne, rows, Ds)
        outg[:, :, pl.ds(pl.multiple_of(j * Ds, 128), Ds)] = sent
        return carry

    lax.fori_loop(0, ne, normalise, 0)

    def dispatch(k):
        to = (me + k) % ne
        return remote(outg.at[to], arr.at[me], a_send.at[k - 1], a_recv.at[k - 1], expert=to)

    def give_back(k):
        to = (me + k) % ne
        return remote(outc.at[to], ret.at[me], b_send.at[k - 1], b_recv.at[k - 1], expert=to)

    for k in range(1, ne):
        dispatch(k).start()
    arr[me] = outg[me]

    g_acc[...] = product(xn[me], sg[me])
    u_acc[...] = product(xn[me], su[me])

    def shared(s):
        a, b = at(pos - s - 1), at(pos + s + 1)
        g_acc[...] += product(xn[a], sg[a])
        u_acc[...] += product(xn[b], su[b])

    ring(1)
    ring(2)
    for copy in experts:
        copy.wait()
    for k in range(1, ne):
        dispatch(k).wait_recv()
    eg_acc[...] = jnp.zeros_like(eg_acc)
    eu_acc[...] = jnp.zeros_like(eu_acc)

    def expert_in(j, carry):
        depth = pl.ds(pl.multiple_of(j * Ds, 128), Ds)
        v = arr[:, :, depth].reshape(ne * rows, Ds)
        eg_acc[...] += product(v, eg[depth, :])
        eu_acc[...] += product(v, eu[depth, :])
        return carry

    lax.fori_loop(0, ne // 2, expert_in, 0)
    ring(3)
    lax.fori_loop(ne // 2, ne, expert_in, 0)
    ehid[...] = (silu(eg_acc[...]) * eu_acc[...]).astype(BF16)

    def expert_out(j, carry):
        width = pl.ds(pl.multiple_of(j * Ds, 128), Ds)
        outc[:, :, width] = product(ehid[...], ed[:, width]).astype(BF16).reshape(ne, rows, Ds)
        return carry

    lax.fori_loop(0, ne, expert_out, 0)
    for k in range(1, ne):
        give_back(k).start()
    ret[me] = outc[me]
    for s in range(4, ne - 1):
        ring(s)
        if s < ne - 2:
            if s == 4:
                for q in range(4):
                    shared(q)
            shared(s)

    @pl.when(pipe == 0)
    def _():
        pl.semaphore_signal(go_sem, inc=1, device_id={"pipe": 1 - pipe}, device_id_type=MESH)

    shared(ne - 2)
    hid[...] = (silu(g_acc[...]) * u_acc[...]).astype(BF16)
    for k in range(1, ne):
        give_back(k).wait_recv()
    weights = combine[...]
    high = weights.astype(BF16)
    low = (weights - high.astype(F32)).astype(BF16)

    def terms(j):
        v = ret[:, :, pl.ds(pl.multiple_of(j * Ds, 128), Ds)].reshape(ne * rows, Ds)
        return product(hid[...], sd[j]) + (product(high, v) + product(low, v))

    def r_copy(k, i):
        to = (ten + k) % nt
        slot = (k - 1) * spt + i
        return remote(y.at[slot], rs.at[slot], r_send.at[slot], r_recv.at[slot], tensor=to)

    for k in range(1, nt):
        for i in range(spt):
            y[(k - 1) * spt + i] = terms(((ten + k) % nt) * spt + i).astype(BF16)
            r_copy(k, i).start()

    for i in range(spt):
        value = xs[base + i].astype(F32) + terms(base + i)
        for k in range(1, nt):
            r_copy(k, i).wait_recv()
            value += rs[(k - 1) * spt + i].astype(F32)
        value = value.astype(BF16)
        res[i] = value
        out[:, i * Ds:(i + 1) * Ds] = value

        @pl.when(pipe == 0)
        def _():
            remote(res.at[i], xs.at[base + i], p_send.at[i], p_recv.at[i], pipe=1 - pipe).start()

    for s in range(ne - 1):
        for make in (gate_copy, up_copy, down_a, down_b):
            make(s).wait_send()
    for k in range(1, ne):
        dispatch(k).wait_send()
        give_back(k).wait_send()
    for k in range(1, nt):
        for i in range(spt):
            x_copy(k, i).wait_send()
            r_copy(k, i).wait_send()

    @pl.when(pipe == 0)
    def _():
        for i in range(spt):
            remote(res.at[i], xs.at[base + i], p_send.at[i], p_recv.at[i], pipe=1 - pipe).wait_send()


def per_device(
    tokens, norm_gain, shared_gate, shared_up, shared_down,
    expert_gate, expert_up, expert_down, expert_ids, expert_slots, route_weights,
):
    ne = lax.axis_size("expert")
    nt = lax.axis_size("tensor")
    batches, block, width = tokens.shape
    T = batches * block
    D = width * nt
    Ds = shared_gate.shape[1]
    F = shared_gate.shape[2]
    FE = expert_gate.shape[3]
    spt = ne // nt
    rows = -(-batches * CAP // 16) * 16

    ids, slots, weights = expert_ids[0], expert_slots[0], route_weights[0]
    valid = (ids < ne) & (slots >= 0)
    batch = jnp.arange(batches, dtype=jnp.int32)[:, None, None]
    code = jnp.where(valid, ids * rows + batch * CAP + slots, -1).reshape(T, -1)
    matched = code[:, :, None] == jnp.arange(ne * rows, dtype=jnp.int32)[None, None, :]
    picker = jnp.any(matched, axis=1).T.astype(BF16)
    combine = jnp.sum(jnp.where(matched, weights.reshape(T, -1)[:, :, None], F32(0.0)), axis=1)

    vmem = pl.BlockSpec(memory_space=pltpu.VMEM)
    hbm = pl.BlockSpec(memory_space=pl.ANY)
    dma = pltpu.SemaphoreType.DMA
    steps = ne - 1
    others = max(nt - 1, 1)
    out = pl.pallas_call(
        functools.partial(layer_kernel, ne, nt),
        out_shape=jax.ShapeDtypeStruct((T, width), BF16),
        in_specs=[hbm, vmem, vmem, vmem] + [hbm] * 6,
        out_specs=vmem,
        scratch_shapes=[
            pltpu.VMEM((ne, T, Ds), BF16),
            pltpu.VMEM((ne, T, Ds), BF16),
            pltpu.VMEM((ne, Ds, F), BF16),
            pltpu.VMEM((ne, Ds, F), BF16),
            pltpu.VMEM((ne, F, Ds), BF16),
            pltpu.VMEM((D, FE), BF16),
            pltpu.VMEM((D, FE), BF16),
            pltpu.VMEM((FE, D), BF16),
            pltpu.VMEM((ne, rows, D), BF16),
            pltpu.VMEM((ne, rows, D), BF16),
            pltpu.VMEM((ne, rows, D), BF16),
            pltpu.VMEM((ne, rows, D), BF16),
            pltpu.VMEM((T, F), F32),
            pltpu.VMEM((T, F), F32),
            pltpu.VMEM((T, F), BF16),
            pltpu.VMEM((ne * rows, FE), F32),
            pltpu.VMEM((ne * rows, FE), F32),
            pltpu.VMEM((ne * rows, FE), BF16),
            pltpu.VMEM((others * spt, T, Ds), BF16),
            pltpu.VMEM((others * spt, T, Ds), BF16),
            pltpu.VMEM((spt, T, Ds), BF16),
            dma((2, steps)), dma((2, steps)), dma((2, steps)), dma((2, steps)),
            dma((others, spt)), dma((others, spt)),
            dma((steps,)), dma((steps,)), dma((steps,)), dma((steps,)),
            dma((others * spt,)), dma((others * spt,)),
            dma((spt,)), dma((spt,)),
            dma((3,)), dma((3,)), dma((spt,)),
            pltpu.SemaphoreType.REGULAR,
        ],
        compiler_params=pltpu.CompilerParams(
            collective_id=0, has_side_effects=True, vmem_limit_bytes=60 * 1024 * 1024
        ),
    )(
        tokens.reshape(T, width), norm_gain[0].reshape(ne, 1, Ds), picker, combine,
        shared_gate[0], shared_up[0], shared_down[0],
        expert_gate[0, 0], expert_up[0, 0], expert_down[0, 0],
    )
    return out.reshape(1, batches, block, width)


def solution(mesh):
    in_specs = (
        P(None, "expert", "tensor"),
        P("pipe", None),
        P("pipe", "expert", "tensor"),
        P("pipe", "expert", "tensor"),
        P("pipe", "tensor", "expert"),
        P("pipe", "expert", None, "tensor"),
        P("pipe", "expert", None, "tensor"),
        P("pipe", "expert", "tensor", None),
        P("pipe", None, "expert", None),
        P("pipe", None, "expert", None),
        P("pipe", None, "expert", None),
    )
    out_specs = P("pipe", None, "expert", "tensor")
    return jax.shard_map(
        per_device, mesh=mesh, in_specs=in_specs, out_specs=out_specs, check_vma=False
    )
```

```python
import functools

import jax
import jax.numpy as jnp
from jax import lax
from jax.experimental import pallas as pl
from jax.experimental.pallas import tpu as pltpu
from jax.sharding import PartitionSpec as P

CAP = 3
GATE_PIECES = 2
DOWN_PIECES = 1
EARLY = (0.15, 0.24, 0.45)
EXPERT_END = 0.88
LAST = 0.9
MESH = pl.DeviceIdType.MESH
F32 = jnp.float32
BF16 = jnp.bfloat16


def product(left, right):
    return jnp.dot(left, right, preferred_element_type=F32)


def silu(value):
    return value / (1.0 + jnp.exp(-value))


def layer_kernel(
    ne, nt,
    x_hbm, gain, picker, combine, sg_hbm, su_hbm, sd_hbm, eg_hbm, eu_hbm, ed_hbm,
    out,
    xs, xn, sg, su, sd, eg, eu, ed,
    outg, arr, outc, ret, hy, hr, g_acc, u_acc, hid, eg_acc, eu_acc, ehid, y, rs, res,
    w_send, w_recv, d_send, d_recv, x_send, x_recv, a_send, a_recv, b_send, b_recv,
    f_send, f_recv, h_send, h_recv, r_send, r_recv, p_send, p_recv, own_sem, exp_sem, x_sem, go_sem,
):
    pipe = lax.axis_index("pipe")
    ten = lax.axis_index("tensor")
    me = lax.axis_index("expert")
    spt = ne // nt
    T, Ds = xs.shape[1], xs.shape[2]
    F = sg.shape[2]
    rows = outg.shape[1]
    half = F // 2
    base = ten * spt

    odd = me % 2
    pos = (1 - odd) * (me // 2) + odd * (ne - 1 - me // 2)

    def at(p):
        p = (p + 2 * ne) % ne
        upper = p // (ne // 2)
        return (1 - upper) * (2 * p) + upper * (2 * (ne - 1 - p) + 1)

    def remote(src, dst, send, recv, **device):
        return pltpu.make_async_remote_copy(
            src_ref=src, dst_ref=dst, send_sem=send, recv_sem=recv,
            device_id=device, device_id_type=MESH,
        )

    barrier = pltpu.get_barrier_semaphore()
    for k in range(1, ne):
        pl.semaphore_signal(barrier, inc=1, device_id={"expert": (me + k) % ne}, device_id_type=MESH)
    for k in range(1, nt):
        pl.semaphore_signal(barrier, inc=1, device_id={"tensor": (ten + k) % nt}, device_id_type=MESH)
    pl.semaphore_signal(barrier, inc=1, device_id={"pipe": 1 - pipe}, device_id_type=MESH)

    own = [
        pltpu.make_async_copy(sg_hbm, sg.at[me], own_sem.at[0]),
        pltpu.make_async_copy(su_hbm, su.at[me], own_sem.at[1]),
        pltpu.make_async_copy(sd_hbm, sd.at[me], own_sem.at[2]),
    ]
    for copy in own:
        copy.start()
    x_in = [
        pltpu.make_async_copy(x_hbm.at[:, pl.ds(i * Ds, Ds)], xs.at[base + i], x_sem.at[i])
        for i in range(spt)
    ]

    @pl.when(pipe == 0)
    def _():
        for copy in x_in:
            copy.start()

    experts = [
        pltpu.make_async_copy(eg_hbm, eg, exp_sem.at[0]),
        pltpu.make_async_copy(eu_hbm, eu, exp_sem.at[1]),
        pltpu.make_async_copy(ed_hbm, ed, exp_sem.at[2]),
    ]
    for copy in experts:
        copy.start()
    pl.semaphore_wait(barrier, ne - 1 + nt - 1 + 1)

    right, left = at(pos + 1), at(pos - 1)

    gate_rows, down_rows = Ds // GATE_PIECES, half // DOWN_PIECES

    def gate_copy(s, p):
        block = sg.at[at(pos - s), pl.ds(p * gate_rows, gate_rows)]
        return remote(block, block, w_send.at[0, s, p], w_recv.at[0, s, p], expert=right)

    def up_copy(s, p):
        block = su.at[at(pos + s), pl.ds(p * gate_rows, gate_rows)]
        return remote(block, block, w_send.at[1, s, p], w_recv.at[1, s, p], expert=left)

    def down_a(s, p):
        block = sd.at[at(pos - s), pl.ds(p * down_rows, down_rows)]
        return remote(block, block, d_send.at[0, s, p], d_recv.at[0, s, p], expert=right)

    def down_b(s, p):
        block = sd.at[at(pos + s), pl.ds(half + p * down_rows, down_rows)]
        return remote(block, block, d_send.at[1, s, p], d_recv.at[1, s, p], expert=left)

    pieces = [(make, p) for p in range(GATE_PIECES) for make in (gate_copy, up_copy)]
    pieces += [(make, p) for p in range(DOWN_PIECES) for make in (down_a, down_b)]
    events = [(s, make, p) for s in range(ne - 1) for make, p in pieces]

    def ring(begin, end):
        for s, make, p in events[int(begin * len(events)):int(end * len(events))]:
            make(s, p).wait_recv()
            if s + 1 < ne - 1:
                make(s + 1, p).start()

    @pl.when(pipe == 1)
    def _():
        pl.semaphore_wait(go_sem, 1)

    for copy in own:
        copy.wait()
    for make, p in pieces:
        make(0, p).start()

    @pl.when(pipe == 0)
    def _():
        for copy in x_in:
            copy.wait()

    @pl.when(pipe == 1)
    def _():
        ring(0.0, EARLY[-1])
        for i in range(spt):
            block = xs.at[base + i]
            remote(block, block, p_send.at[i], p_recv.at[i], pipe=1 - pipe).wait_recv()

    def x_copy(k, i):
        block = xs.at[base + i]
        return remote(block, block, x_send.at[k - 1, i], x_recv.at[k - 1, i], tensor=(ten + k) % nt)

    for k in range(1, nt):
        for i in range(spt):
            x_copy(k, i).start()

    @pl.when(pipe == 0)
    def _():
        ring(0.0, EARLY[0])

    for k in range(1, nt):
        for i in range(spt):
            x_copy(k, i).wait_recv()

    def squares(j, total):
        v = xs[j].astype(F32)
        return total + jnp.sum(v * v, axis=-1, keepdims=True)

    total = lax.fori_loop(0, ne, squares, jnp.zeros((T, 1), F32))
    inverse = lax.rsqrt(total / (ne * Ds) + 1e-06)

    def column(i):
        return pl.ds(pl.multiple_of(i * Ds, 128), Ds)

    def normed(j):
        v = (xs[j].astype(F32) * inverse * gain[j]).astype(BF16)
        xn[j] = v
        return v

    def normalise_own(i, carry):
        sent = product(picker[...], normed(base + i)).astype(BF16)
        outg[:, :, column(i)] = sent.reshape(ne, rows, Ds)
        return carry

    lax.fori_loop(0, spt, normalise_own, 0)

    def dispatch(k):
        to = (me + k) % ne
        return remote(outg.at[to], arr.at[ten, me], a_send.at[k - 1], a_recv.at[k - 1], expert=to)

    def spread(q, k):
        block = arr.at[ten, (me + ne - k) % ne]
        return remote(block, block, f_send.at[q - 1, k], f_recv.at[q - 1, k], tensor=(ten + q) % nt)

    def give_back(k):
        to = (me + k) % ne
        return remote(outc.at[to], ret.at[me], b_send.at[k - 1], b_recv.at[k - 1], expert=to)

    for k in range(1, ne):
        dispatch(k).start()
    arr[ten, me] = outg[me]
    for q in range(1, nt):
        spread(q, 0).start()

    @pl.when(pipe == 0)
    def _():
        ring(EARLY[0], EARLY[1])

    def normalise_others(j, carry):
        normed((base + spt + j) % ne)
        return carry

    lax.fori_loop(0, ne - spt, normalise_others, 0)
    g_acc[...] = product(xn[me], sg[me])
    u_acc[...] = product(xn[me], su[me])

    def shared(s):
        a, b = at(pos - s - 1), at(pos + s + 1)
        g_acc[...] += product(xn[a], sg[a])
        u_acc[...] += product(xn[b], su[b])

    @pl.when(pipe == 0)
    def _():
        ring(EARLY[1], EARLY[2])

    for copy in experts:
        copy.wait()
    for k in range(1, ne):
        dispatch(k).wait_recv()
        for q in range(1, nt):
            spread(q, k).start()
    ticks = [EARLY[2]]

    def tick():
        later = ticks[0] + (EXPERT_END - EARLY[2]) / (4 * ne)
        ring(ticks[0], later)
        ticks[0] = later

    eg_acc[...] = jnp.zeros_like(eg_acc)
    eu_acc[...] = jnp.zeros_like(eu_acc)

    def expert_in(group):
        for i in range(spt):
            depth = pl.ds(pl.multiple_of(group * (spt * Ds) + i * Ds, 128), Ds)
            v = arr[group, :, :, i * Ds:(i + 1) * Ds].reshape(ne * rows, Ds)
            eg_acc[...] += product(v, eg[depth, :])
            tick()
            eu_acc[...] += product(v, eu[depth, :])
            tick()

    expert_in(ten)
    for q in range(1, nt):
        for k in range(ne):
            spread(q, k).wait_recv()
        expert_in((ten + q) % nt)
    ehid[...] = (silu(eg_acc[...]) * eu_acc[...]).astype(BF16)

    def h_copy(q, i):
        slot = (q - 1) * spt + i
        return remote(hy.at[slot], hr.at[slot], h_send.at[slot], h_recv.at[slot], tensor=(ten + q) % nt)

    def expert_out(group, i):
        return product(ehid[...], ed[:, pl.ds(pl.multiple_of(group * (spt * Ds) + i * Ds, 128), Ds)])

    for q in range(1, nt):
        for i in range(spt):
            hy[(q - 1) * spt + i] = expert_out((ten + q) % nt, i).astype(BF16)
            h_copy(q, i).start()
            tick()
            tick()
    for i in range(spt):
        value = expert_out(ten, i)
        for q in range(1, nt):
            h_copy(q, i).wait_recv()
            value += hr[(q - 1) * spt + i].astype(F32)
        outc[:, :, i * Ds:(i + 1) * Ds] = value.astype(BF16).reshape(ne, rows, Ds)
        tick()
        tick()
    for k in range(1, ne):
        give_back(k).start()
    ret[me] = outc[me]
    held = ticks[0]
    for s in range(ne - 2):
        later = max(held, min(held + (LAST - held) * (s + 1) / (ne - 3), (s + 2) / (ne - 1), 1.0))
        if s == ne - 3:
            @pl.when(pipe == 0)
            def _():
                pl.semaphore_signal(go_sem, inc=1, device_id={"pipe": 1 - pipe}, device_id_type=MESH)

            later = 1.0
        ring(held, max(held, (s + 1) / (ne - 1)))
        held = max(held, (s + 1) / (ne - 1))
        shared(s)
        ring(held, max(held, later))
        held = max(held, later)
    shared(ne - 2)
    hid[...] = (silu(g_acc[...]) * u_acc[...]).astype(BF16)

    def terms(j):
        return product(hid[...], sd[j])

    def r_copy(k, i):
        to = (ten + k) % nt
        slot = (k - 1) * spt + i
        return remote(y.at[slot], rs.at[slot], r_send.at[slot], r_recv.at[slot], tensor=to)

    for k in range(1, nt):
        for i in range(spt):
            y[(k - 1) * spt + i] = terms(((ten + k) % nt) * spt + i).astype(BF16)
            r_copy(k, i).start()

    for k in range(1, ne):
        give_back(k).wait_recv()
    weights = combine[...]
    high = weights.astype(BF16)
    low = (weights - high.astype(F32)).astype(BF16)
    for i in range(spt):
        v = ret[:, :, i * Ds:(i + 1) * Ds].reshape(ne * rows, Ds)
        value = xs[base + i].astype(F32) + terms(base + i) + (product(high, v) + product(low, v))
        for k in range(1, nt):
            r_copy(k, i).wait_recv()
            value += rs[(k - 1) * spt + i].astype(F32)
        value = value.astype(BF16)
        res[i] = value
        out[:, i * Ds:(i + 1) * Ds] = value

        @pl.when(pipe == 0)
        def _():
            remote(res.at[i], xs.at[base + i], p_send.at[i], p_recv.at[i], pipe=1 - pipe).start()

    for s in range(ne - 1):
        for make, p in pieces:
            make(s, p).wait_send()
    for k in range(1, ne):
        dispatch(k).wait_send()
        give_back(k).wait_send()
    for k in range(1, nt):
        for i in range(spt):
            x_copy(k, i).wait_send()
            r_copy(k, i).wait_send()
            h_copy(k, i).wait_send()
        for i in range(ne):
            spread(k, i).wait_send()

    @pl.when(pipe == 0)
    def _():
        for i in range(spt):
            remote(res.at[i], xs.at[base + i], p_send.at[i], p_recv.at[i], pipe=1 - pipe).wait_send()


def per_device(
    tokens, norm_gain, shared_gate, shared_up, shared_down,
    expert_gate, expert_up, expert_down, expert_ids, expert_slots, route_weights,
):
    ne = lax.axis_size("expert")
    nt = lax.axis_size("tensor")
    batches, block, width = tokens.shape
    T = batches * block
    D = width * nt
    Ds = shared_gate.shape[1]
    F = shared_gate.shape[2]
    FE = expert_gate.shape[3]
    spt = ne // nt
    rows = -(-batches * CAP // 16) * 16

    ids, slots, weights = expert_ids[0], expert_slots[0], route_weights[0]
    valid = (ids < ne) & (slots >= 0)
    batch = jnp.arange(batches, dtype=jnp.int32)[:, None, None]
    code = jnp.where(valid, ids * rows + batch * CAP + slots, -1).reshape(T, -1)
    matched = code[:, :, None] == jnp.arange(ne * rows, dtype=jnp.int32)[None, None, :]
    picker = jnp.any(matched, axis=1).T.astype(BF16)
    combine = jnp.sum(jnp.where(matched, weights.reshape(T, -1)[:, :, None], F32(0.0)), axis=1)

    vmem = pl.BlockSpec(memory_space=pltpu.VMEM)
    hbm = pl.BlockSpec(memory_space=pl.ANY)
    dma = pltpu.SemaphoreType.DMA
    steps = ne - 1
    others = max(nt - 1, 1)
    out = pl.pallas_call(
        functools.partial(layer_kernel, ne, nt),
        out_shape=jax.ShapeDtypeStruct((T, width), BF16),
        in_specs=[hbm, vmem, vmem, vmem] + [hbm] * 6,
        out_specs=vmem,
        scratch_shapes=[
            pltpu.VMEM((ne, T, Ds), BF16),
            pltpu.VMEM((ne, T, Ds), BF16),
            pltpu.VMEM((ne, Ds, F), BF16),
            pltpu.VMEM((ne, Ds, F), BF16),
            pltpu.VMEM((ne, F, Ds), BF16),
            pltpu.VMEM((D, FE), BF16),
            pltpu.VMEM((D, FE), BF16),
            pltpu.VMEM((FE, D), BF16),
            pltpu.VMEM((ne, rows, width), BF16),
            pltpu.VMEM((nt, ne, rows, width), BF16),
            pltpu.VMEM((ne, rows, width), BF16),
            pltpu.VMEM((ne, rows, width), BF16),
            pltpu.VMEM((others * spt, ne * rows, Ds), BF16),
            pltpu.VMEM((others * spt, ne * rows, Ds), BF16),
            pltpu.VMEM((T, F), F32),
            pltpu.VMEM((T, F), F32),
            pltpu.VMEM((T, F), BF16),
            pltpu.VMEM((ne * rows, FE), F32),
            pltpu.VMEM((ne * rows, FE), F32),
            pltpu.VMEM((ne * rows, FE), BF16),
            pltpu.VMEM((others * spt, T, Ds), BF16),
            pltpu.VMEM((others * spt, T, Ds), BF16),
            pltpu.VMEM((spt, T, Ds), BF16),
            dma((2, steps, GATE_PIECES)), dma((2, steps, GATE_PIECES)),
            dma((2, steps, DOWN_PIECES)), dma((2, steps, DOWN_PIECES)),
            dma((others, spt)), dma((others, spt)),
            dma((steps,)), dma((steps,)), dma((steps,)), dma((steps,)),
            dma((others, ne)), dma((others, ne)),
            dma((others * spt,)), dma((others * spt,)),
            dma((others * spt,)), dma((others * spt,)),
            dma((spt,)), dma((spt,)),
            dma((3,)), dma((3,)), dma((spt,)),
            pltpu.SemaphoreType.REGULAR,
        ],
        compiler_params=pltpu.CompilerParams(
            collective_id=0, has_side_effects=True, vmem_limit_bytes=60 * 1024 * 1024
        ),
    )(
        tokens.reshape(T, width), norm_gain[0].reshape(ne, 1, Ds), picker, combine,
        shared_gate[0], shared_up[0], shared_down[0],
        expert_gate[0, 0], expert_up[0, 0], expert_down[0, 0],
    )
    return out.reshape(1, batches, block, width)


def solution(mesh):
    in_specs = (
        P(None, "expert", "tensor"),
        P("pipe", None),
        P("pipe", "expert", "tensor"),
        P("pipe", "expert", "tensor"),
        P("pipe", "tensor", "expert"),
        P("pipe", "expert", None, "tensor"),
        P("pipe", "expert", None, "tensor"),
        P("pipe", "expert", "tensor", None),
        P("pipe", None, "expert", None),
        P("pipe", None, "expert", None),
        P("pipe", None, "expert", None),
    )
    out_specs = P("pipe", None, "expert", "tensor")
    return jax.shard_map(
        per_device, mesh=mesh, in_specs=in_specs, out_specs=out_specs, check_vma=False
    )
```
